32 devices in a mesh: row: 16 (over z, x, core), chan: 2 (over y).
Axes of the slice: x: 2, y: 2, z: 4, core: 2. Of those that a mesh axis runs over, the one named last changes fastest.
Arguments:
- pair_rep: float32 [256, 256, 128], P('row', 'chan'), may hold values from -630 to 630
- residue_mask: int32 [256], replicated, may hold values from 0 to 1, as said below
- norm_gain: float32 [128], replicated, may hold values from 0.5 to 1.5
- norm_shift: float32 [128], replicated, may hold values from -3 to 3
- proj_weight: float32 [128, 512], replicated, may hold values from -4 to 4
- gate_shift: float32 [128], replicated, may hold values from -4 to 4
- bias_weight: float32 [128, 4], replicated, may hold values from -0.5 to 0.5
- out_weight: float32 [128, 128], replicated, may hold values from -0.5 to 0.5
Outputs:
- update: float32 [256, 256, 128], P('row', 'chan')
The draws below stay inside these ranges and needn't reach their ends.
Inputs may be any that keep to these rules, and one draw needn't show every extreme that they name: `residue_mask`: residue 0 is always valid.
All inputs are finite; a program needn't handle non-finite values.
Results may differ from the reference program's by a relative error of at most 0.012.
Values may be sent and summed in bfloat16 or wider, within the bound.
No kernel may reach another device: no remote copies, remote signals or barrier semaphores. Data moves between devices by JAX's collectives and lax.ppermute only.
A program may use at most 64 MiB of HBM per device.

```python
import math
import jax
import jax.numpy as jnp
from jax import lax

C = 128
HEADS = 4
N = 256


def draw_pair_rep(key, part):
    key_noise, key_chan, key_pos = jax.random.split(key, 3)
    noise_draw = jnp.clip(jax.random.normal(key_noise, (N, N, C), jnp.float32), -6.0, 6.0)
    chan_scale = 10.0 ** jax.random.uniform(key_chan, (C,), jnp.float32)
    pos_scale = 10.0 ** jax.random.uniform(key_pos, (N, N, 1), jnp.float32)
    return noise_draw * chan_scale * pos_scale


def draw_proj_weight(key, part):
    key_base = jax.random.fold_in(key, 0)
    base = jnp.clip(jax.random.normal(key_base, (C, 4, HEADS, C // HEADS), jnp.float32), -4.0, 4.0) / math.sqrt(C)
    return base.reshape(C, 4 * C)


def draw_residue_mask(key, part):
    levels = jax.random.randint(key, (N,), 0, 4)
    return jnp.where(levels > 0, 1, 0).astype(jnp.int32).at[0].set(1)


def centred(own_key, extent, width, limit, dtype=jnp.bfloat16):
    result = width * jax.random.normal(own_key, extent, jnp.float32)
    return jnp.clip(result, min=-limit, max=limit).astype(dtype)


def setup_inputs(seed: int = 0) -> dict:
    splits = jax.random.split(jax.random.key(seed), 9)
    pair_rep = draw_pair_rep(jax.random.fold_in(splits[8], 71), 0)
    residue_mask = draw_residue_mask(jax.random.fold_in(splits[8], 71), 0)
    norm_gain = jnp.clip(1.0 + 0.1 * jax.random.normal(splits[2], (C,), jnp.float32), 0.5, 1.5)
    norm_shift = centred(splits[3], (C,), 0.5, 3.0, jnp.float32)
    proj_weight = draw_proj_weight(jax.random.fold_in(splits[8], 71), 0)
    gate_shift = centred(splits[5], (C,), 1.0, 4.0, jnp.float32)
    bias_weight = centred(splits[6], (C, HEADS), C ** -0.5, 0.5, jnp.float32)
    out_weight = centred(splits[7], (C, C), C ** -0.5, 0.5, jnp.float32)
    return {"pair_rep": pair_rep, "residue_mask": residue_mask, "norm_gain": norm_gain, "norm_shift": norm_shift, "proj_weight": proj_weight, "gate_shift": gate_shift, "bias_weight": bias_weight, "out_weight": out_weight}


def normalize(values, norm_gain, norm_shift):
    average = lax.optimization_barrier(jnp.mean(values, axis=-1, keepdims=True))
    centered = values - average
    variance = lax.optimization_barrier(jnp.mean(centered * centered, axis=-1, keepdims=True))
    return centered * lax.rsqrt(variance + 1e-05) * norm_gain + norm_shift

def reference(pair_rep, residue_mask, norm_gain, norm_shift, proj_weight, gate_shift, bias_weight, out_weight):
    highest = lax.Precision.HIGHEST
    head_dim = C // HEADS
    scaling = 1.0 / math.sqrt(head_dim)
    normed = normalize(pair_rep, norm_gain, norm_shift)
    pair_bias = jnp.einsum('jkc,ch->hjk', normed, bias_weight, precision=highest)
    valid_keys = (residue_mask > 0)[None, None, :]

    def one_row(pair_row):
        projected = jnp.dot(pair_row, proj_weight, precision=highest)
        query_half = (projected[:, :C] * scaling).astype(jnp.bfloat16)
        key_half = projected[:, C:2 * C].astype(jnp.bfloat16)
        value_half = projected[:, 2 * C:3 * C].astype(jnp.bfloat16)
        gates = projected[:, 3 * C:]
        queries = query_half.astype(jnp.float32).reshape(N, HEADS, head_dim)
        key_rows = key_half.astype(jnp.float32).reshape(N, HEADS, head_dim)
        value_rows = value_half.astype(jnp.float32).reshape(N, HEADS, head_dim)
        scores = jnp.einsum('jhd,khd->hjk', queries, key_rows, precision=highest) + pair_bias
        scores = jnp.where(valid_keys, scores, -1000000000.0)
        weights = jax.nn.softmax(scores, axis=-1)
        attended = jnp.einsum('hjk,khd->jhd', weights, value_rows, precision=highest).reshape(N, C)
        gated_rows = jax.nn.sigmoid(gates + gate_shift) * attended
        return jnp.dot(gated_rows, out_weight, precision=highest)
    return lax.map(one_row, normed)
```

```python
import math

import jax
import jax.numpy as jnp
from jax import lax
from jax.experimental import pallas as pl
from jax.experimental.pallas import tpu as pltpu
from jax.sharding import PartitionSpec as P

HEADS = 4
CHUNKS = 1
STEP_ROWS = 4
LOG2E = 1.4426950408889634


VMEM = pl.BlockSpec(memory_space=pltpu.VMEM)
SMEM = pl.BlockSpec(memory_space=pltpu.SMEM)


def dot(a, b, dims):
    return lax.dot_general(a, b, (dims, ((), ())), preferred_element_type=jnp.float32)


def split(values):
    high = values.astype(jnp.bfloat16)
    return high, (values - high.astype(jnp.float32)).astype(jnp.bfloat16)


def norm_kernel(pair_ref, gain_ref, shift_ref, bias_weight_ref, *refs):
    *normed_refs, bias_ref, scratch = refs
    pair_rows, span, width = pair_ref.shape
    chunk_rows = normed_refs[0].shape[0]
    weight_t = jnp.transpose(bias_weight_ref[...])
    high, low = split(weight_t)
    weights = jnp.concatenate([high, high], axis=1)
    low_weights = jnp.concatenate([low, jnp.zeros_like(low)], axis=1)
    gain = gain_ref[...]
    shift = shift_ref[...]
    for row in range(pair_rows):
        values = pair_ref[row]
        average = jnp.mean(values, axis=-1, keepdims=True)
        centered = values - average
        variance = jnp.mean(centered * centered, axis=-1, keepdims=True)
        normed, rest = split(centered * lax.rsqrt(variance + 1e-05) * gain + shift)
        normed_refs[row // chunk_rows][row % chunk_rows] = normed
        both = jnp.concatenate([normed, rest], axis=1)
        bias = dot(weights, both, ((1,), (1,))) + dot(low_weights, both, ((1,), (1,)))
        for head in range(HEADS):
            scratch[pl.ds(head * pair_rows + row, 1), :] = bias[head : head + 1, :]
    bias_ref[...] = scratch[...].astype(jnp.bfloat16)


def prepare_kernel(
    chan_ref, row_ref, gathered_ref, mask_ref, proj_ref, gate_shift_ref, out_weight_ref,
    bias_ref, qgv_ref, key_ref, out_ref, gate_ref,
):
    spans = mask_ref.shape[0]
    span = mask_ref.shape[2]
    width = proj_ref.shape[0]
    pair_rows = gathered_ref.shape[1] // HEADS
    group = span // pair_rows
    place = chan_ref[0]
    part = lax.rem(row_ref[0], group)
    top = lax.div(row_ref[0], group)
    bits = group.bit_length() - 1
    slots = []
    for q in range(group):
        apart = part ^ q
        slots.append(
            sum(((apart >> bit) & 1) << (bits - 1 - bit) for bit in range(bits)) * spans
        )
    for shift in range(spans):
        source = lax.rem(place + shift, spans)
        passed = lax.rem(top - source + spans, spans)
        valid = mask_ref[source] > 0
        for head in range(HEADS):
            pieces = [
                gathered_ref[slot + passed, head * pair_rows : (head + 1) * pair_rows, :]
                for slot in slots
            ]
            tile = jnp.concatenate(pieces, axis=0).astype(jnp.float32) * LOG2E
            tile = jnp.where(valid, tile, -1e9)
            bias_ref[shift * span : (shift + 1) * span, head * span : (head + 1) * span] = (
                jnp.transpose(tile)
            )
    scaling = LOG2E / math.sqrt(width // HEADS)
    blocks = [
        proj_ref[:, :width] * scaling,
        proj_ref[:, 3 * width :],
        proj_ref[:, 2 * width : 3 * width],
    ]
    for place, weight in enumerate(blocks):
        rows = slice(place * width, (place + 1) * width)
        qgv_ref[rows, :width], qgv_ref[rows, width:] = split(jnp.transpose(weight))
    key_ref[:width], key_ref[width:] = split(proj_ref[:, width : 2 * width])
    out_ref[:width], out_ref[2 * width :] = split(out_weight_ref[...])
    out_ref[width : 2 * width] = out_ref[:width]
    gate_ref[...] = jnp.transpose(jnp.broadcast_to(gate_shift_ref[...], (span, width)))


def attend_kernel(
    bias_ref, qgv_ref, key_ref, out_weight_ref, gate_ref, *rest
):
    *normed_refs, update_ref = rest
    rows, span, width = normed_refs[0].shape
    head_dim = width // HEADS
    nothing = jnp.zeros((head_dim, span), jnp.bfloat16)
    for row in range(rows):
        every = jnp.concatenate([ref[row] for ref in normed_refs], axis=0)
        every = jnp.concatenate([every, every], axis=1)
        own = every[:span]
        query_gate = dot(qgv_ref[: 2 * width], own, ((1,), (1,)))
        values = dot(qgv_ref[2 * width :], every, ((1,), (1,))).astype(jnp.bfloat16)
        keys = dot(every, key_ref[...], ((1,), (0,))).astype(jnp.bfloat16)
        query = query_gate[:width].astype(jnp.bfloat16)
        spread = jnp.concatenate(
            [
                jnp.concatenate(
                    [
                        query[head * head_dim : (head + 1) * head_dim] if other == head else nothing
                        for other in range(HEADS)
                    ],
                    axis=0,
                )
                for head in range(HEADS)
            ],
            axis=1,
        )
        scores = dot(keys, spread, ((1,), (0,))) + bias_ref[...]
        powers = jnp.exp2(scores - jnp.max(scores, axis=0, keepdims=True))
        inverse = 1.0 / jnp.sum(powers, axis=0, keepdims=True)
        powers = powers.astype(jnp.bfloat16)
        attended = jnp.concatenate(
            [
                dot(
                    values[head * head_dim : (head + 1) * head_dim],
                    powers[:, head * span : (head + 1) * span],
                    ((1,), (0,)),
                )
                * inverse[:, head * span : (head + 1) * span]
                for head in range(HEADS)
            ],
            axis=0,
        )
        gated = jax.nn.sigmoid(query_gate[width:] + gate_ref[...]) * attended
        high, low = split(jnp.transpose(gated))
        update_ref[row] = dot(
            jnp.concatenate([high, low, high], axis=1), out_weight_ref[...], ((1,), (0,))
        )


def spread_bias(bias, devices, spans):
    group = devices // spans

    def flat(top, part, place):
        return (top * group + part) * spans + place

    blocks = [
        lax.ppermute(
            bias,
            ("row", "chan"),
            [
                (flat(top, part, place), flat((place + step) % spans, part, top))
                for top in range(spans)
                for part in range(group)
                for place in range(spans)
            ],
        )
        for step in range(spans)
    ]
    held = jnp.concatenate(blocks, axis=0)
    apart = group // 2
    while apart:
        other = lax.ppermute(held, "row", [(r, r ^ apart) for r in range(devices)])
        held = jnp.concatenate([held, other], axis=0)
        apart //= 2
    return held.reshape(group * spans, *bias.shape)


def make_body(devices, spans):
    def body(
        pair_rep, residue_mask, norm_gain, norm_shift, proj_weight, gate_shift, bias_weight,
        out_weight,
    ):
        pair_rows, span, width = pair_rep.shape
        chunk_rows = pair_rows // CHUNKS
        half = jnp.bfloat16
        *chunks, bias = pl.pallas_call(
            norm_kernel,
            name="norm",
            out_shape=[jax.ShapeDtypeStruct((chunk_rows, span, width), half)] * CHUNKS
            + [jax.ShapeDtypeStruct((HEADS * pair_rows, span), half)],
            in_specs=[VMEM] * 4,
            out_specs=[VMEM] * (CHUNKS + 1),
            scratch_shapes=[pltpu.VMEM((HEADS * pair_rows, span), jnp.float32)],
        )(pair_rep, norm_gain[None], norm_shift[None], bias_weight)
        remote = [
            [
                lax.ppermute(chunk, "chan", [((d + s) % spans, d) for d in range(spans)])
                for s in range(1, spans)
            ]
            for chunk in chunks
        ]
        gathered = spread_bias(bias, devices, spans)
        prepared = pl.pallas_call(
            prepare_kernel,
            name="prepare",
            out_shape=[
                jax.ShapeDtypeStruct((spans * span, HEADS * span), jnp.float32),
                jax.ShapeDtypeStruct((3 * width, 2 * width), half),
                jax.ShapeDtypeStruct((2 * width, width), half),
                jax.ShapeDtypeStruct((3 * width, width), half),
                jax.ShapeDtypeStruct((width, span), jnp.float32),
            ],
            in_specs=[SMEM] * 2 + [VMEM] * 5,
            out_specs=[VMEM] * 5,
        )(
            lax.axis_index("chan")[None], lax.axis_index("row")[None], gathered,
            residue_mask.reshape(spans, 1, span), proj_weight, gate_shift[None], out_weight,
        )
        block = pl.BlockSpec((STEP_ROWS, span, width), lambda i: (i, 0, 0))
        updates = [
            pl.pallas_call(
                attend_kernel,
                name="attend",
                grid=(chunk_rows // STEP_ROWS,),
                out_shape=jax.ShapeDtypeStruct((chunk_rows, span, width), jnp.float32),
                in_specs=[VMEM] * 5 + [block] * spans,
                out_specs=block,
            )(*prepared, own, *others)
            for own, others in zip(chunks, remote)
        ]
        return updates[0] if CHUNKS == 1 else jnp.concatenate(updates, axis=0)

    return body


def solution(mesh):
    return jax.shard_map(
        make_body(mesh.shape["row"], mesh.shape["chan"]),
        mesh=mesh,
        in_specs=(P("row", "chan", None), P(), P(), P(), P(), P(), P(), P()),
        out_specs=P("row", "chan", None),
        check_vma=False,
    )
```

```python
import math

import jax
import jax.numpy as jnp
from jax import lax
from jax.experimental import pallas as pl
from jax.experimental.pallas import tpu as pltpu
from jax.sharding import PartitionSpec as P

HEADS = 4
CHUNKS = 1
STEP_ROWS = 8
LOG2E = 1.4426950408889634


VMEM = pl.BlockSpec(memory_space=pltpu.VMEM)
SMEM = pl.BlockSpec(memory_space=pltpu.SMEM)


def dot(a, b, dims):
    return lax.dot_general(a, b, (dims, ((), ())), preferred_element_type=jnp.float32)


def split(values):
    high = values.astype(jnp.bfloat16)
    return high, (values - high.astype(jnp.float32)).astype(jnp.bfloat16)


def norm_kernel(pair_ref, gain_ref, shift_ref, bias_weight_ref, *refs):
    *normed_refs, bias_ref, scratch = refs
    pair_rows, span, width = pair_ref.shape
    chunk_rows = normed_refs[0].shape[0]
    high, low = split(bias_weight_ref[...])
    weights = jnp.concatenate([high, high], axis=1)
    low_weights = jnp.concatenate([low, jnp.zeros_like(low)], axis=1)
    gain = gain_ref[...]
    shift = shift_ref[...]
    for row in range(pair_rows):
        values = pair_ref[row]
        average = jnp.mean(values, axis=-1, keepdims=True)
        centered = values - average
        variance = jnp.mean(centered * centered, axis=-1, keepdims=True)
        normed, rest = split(centered * lax.rsqrt(variance + 1e-05) * gain + shift)
        normed_refs[row // chunk_rows][row % chunk_rows] = normed
        both = jnp.concatenate([normed, rest], axis=1)
        bias = dot(weights, both, ((1,), (1,))) + dot(low_weights, both, ((1,), (1,)))
        for head in range(HEADS):
            scratch[pl.ds(head * pair_rows + row, 1), :] = bias[head : head + 1, :]
    bias_ref[...] = scratch[...].astype(jnp.bfloat16)


def prepare_kernel(
    chan_ref, row_ref, gathered_ref, mask_ref, proj_ref, gate_shift_ref, out_weight_ref,
    bias_ref, qgv_ref, key_ref, out_ref, gate_ref,
):
    spans = mask_ref.shape[0]
    span = mask_ref.shape[2]
    width = proj_ref.shape[0]
    pair_rows = gathered_ref.shape[1] // HEADS
    group = span // pair_rows
    place = chan_ref[0]
    part = lax.rem(row_ref[0], group)
    top = lax.div(row_ref[0], group)
    bits = group.bit_length() - 1
    slots = []
    for q in range(group):
        apart = part ^ q
        slots.append(
            sum(((apart >> bit) & 1) << (bits - 1 - bit) for bit in range(bits)) * spans
        )
    for shift in range(spans):
        source = lax.rem(place + shift, spans)
        passed = lax.rem(top - source + spans, spans)
        valid = mask_ref[source] > 0
        for head in range(HEADS):
            pieces = [
                gathered_ref[slot + passed, head * pair_rows : (head + 1) * pair_rows, :]
                for slot in slots
            ]
            tile = jnp.concatenate(pieces, axis=0).astype(jnp.float32) * LOG2E
            tile = jnp.where(valid, tile, -1e9)
            bias_ref[shift * span : (shift + 1) * span, head * span : (head + 1) * span] = (
                jnp.transpose(tile)
            )
    scaling = LOG2E / math.sqrt(width // HEADS)
    blocks = [
        proj_ref[:, :width] * scaling,
        proj_ref[:, 3 * width :],
        proj_ref[:, 2 * width : 3 * width],
    ]
    for place, weight in enumerate(blocks):
        rows = slice(place * width, (place + 1) * width)
        qgv_ref[rows, :width], qgv_ref[rows, width:] = split(jnp.transpose(weight))
    key_ref[:width], key_ref[width:] = split(proj_ref[:, width : 2 * width])
    out_ref[:width], out_ref[2 * width :] = split(out_weight_ref[...])
    out_ref[width : 2 * width] = out_ref[:width]
    gate_ref[...] = jnp.transpose(jnp.broadcast_to(gate_shift_ref[...], (span, width)))


def attend_kernel(
    bias_ref, qgv_ref, key_ref, out_weight_ref, gate_ref, *rest
):
    *normed_refs, update_ref = rest
    rows, span, width = normed_refs[0].shape
    head_dim = width // HEADS
    nothing = jnp.zeros((head_dim, span), jnp.bfloat16)
    own = normed_refs[0][...].reshape(rows * span, width)
    every = jnp.concatenate([ref[row] for row in range(rows) for ref in normed_refs], axis=0)
    own = jnp.concatenate([own, own], axis=1)
    every = jnp.concatenate([every, every], axis=1)
    reach = len(normed_refs) * span
    query_gate = dot(qgv_ref[: 2 * width], own, ((1,), (1,)))
    keys = dot(every, key_ref[...], ((1,), (0,))).astype(jnp.bfloat16)
    values = dot(qgv_ref[2 * width :], every, ((1,), (1,))).astype(jnp.bfloat16)
    gates = jax.nn.sigmoid(
        query_gate[width:] + jnp.concatenate([gate_ref[...]] * rows, axis=1)
    )
    queries = query_gate[:width].astype(jnp.bfloat16)

    def score(row):
        query = queries[:, row * span : (row + 1) * span]
        spread = jnp.concatenate(
            [
                jnp.concatenate(
                    [
                        query[head * head_dim : (head + 1) * head_dim] if other == head else nothing
                        for other in range(HEADS)
                    ],
                    axis=0,
                )
                for head in range(HEADS)
            ],
            axis=1,
        )
        return dot(keys[row * reach : (row + 1) * reach], spread, ((1,), (0,))) + bias_ref[...]

    gated = []
    following = score(0)
    for row in range(rows):
        scores = following
        if row + 1 < rows:
            following = score(row + 1)
        powers = jnp.exp2(scores - jnp.max(scores, axis=0, keepdims=True))
        inverse = 1.0 / jnp.sum(powers, axis=0, keepdims=True)
        powers = powers.astype(jnp.bfloat16)
        attended = jnp.concatenate(
            [
                dot(
                    values[head * head_dim : (head + 1) * head_dim, row * reach : (row + 1) * reach],
                    powers[:, head * span : (head + 1) * span],
                    ((1,), (0,)),
                )
                * inverse[:, head * span : (head + 1) * span]
                for head in range(HEADS)
            ],
            axis=0,
        )
        gated.append(jnp.transpose(gates[:, row * span : (row + 1) * span] * attended))
    high, low = split(jnp.concatenate(gated, axis=0))
    update = dot(jnp.concatenate([high, low, high], axis=1), out_weight_ref[...], ((1,), (0,)))
    update_ref[...] = update.reshape(rows, span, width)


def spread_bias(bias, devices, spans):
    group = devices // spans

    def flat(top, part, place):
        return (top * group + part) * spans + place

    blocks = [
        lax.ppermute(
            bias,
            ("row", "chan"),
            [
                (flat(top, part, place), flat((place + step) % spans, part, top))
                for top in range(spans)
                for part in range(group)
                for place in range(spans)
            ],
        )
        for step in range(spans)
    ]
    held = jnp.concatenate(blocks, axis=0)
    apart = group // 2
    while apart:
        other = lax.ppermute(held, "row", [(r, r ^ apart) for r in range(devices)])
        held = jnp.concatenate([held, other], axis=0)
        apart //= 2
    return held.reshape(group * spans, *bias.shape)


def make_body(devices, spans):
    def body(
        pair_rep, residue_mask, norm_gain, norm_shift, proj_weight, gate_shift, bias_weight,
        out_weight,
    ):
        pair_rows, span, width = pair_rep.shape
        chunk_rows = pair_rows // CHUNKS
        half = jnp.bfloat16
        *chunks, bias = pl.pallas_call(
            norm_kernel,
            name="norm",
            out_shape=[jax.ShapeDtypeStruct((chunk_rows, span, width), half)] * CHUNKS
            + [jax.ShapeDtypeStruct((HEADS * pair_rows, span), half)],
            in_specs=[VMEM] * 4,
            out_specs=[VMEM] * (CHUNKS + 1),
            scratch_shapes=[pltpu.VMEM((HEADS * pair_rows, span), jnp.float32)],
        )(pair_rep, norm_gain[None], norm_shift[None], bias_weight.T)
        remote = [
            [
                lax.ppermute(chunk, "chan", [((d + s) % spans, d) for d in range(spans)])
                for s in range(1, spans)
            ]
            for chunk in chunks
        ]
        gathered = spread_bias(bias, devices, spans)
        prepared = pl.pallas_call(
            prepare_kernel,
            name="prepare",
            out_shape=[
                jax.ShapeDtypeStruct((spans * span, HEADS * span), jnp.float32),
                jax.ShapeDtypeStruct((3 * width, 2 * width), half),
                jax.ShapeDtypeStruct((2 * width, width), half),
                jax.ShapeDtypeStruct((3 * width, width), half),
                jax.ShapeDtypeStruct((width, span), jnp.float32),
            ],
            in_specs=[SMEM] * 2 + [VMEM] * 5,
            out_specs=[VMEM] * 5,
        )(
            lax.axis_index("chan")[None], lax.axis_index("row")[None], gathered,
            residue_mask.reshape(spans, 1, span), proj_weight, gate_shift[None], out_weight,
        )
        block = pl.BlockSpec((STEP_ROWS, span, width), lambda i: (i, 0, 0))
        updates = [
            pl.pallas_call(
                attend_kernel,
                name="attend",
                grid=(chunk_rows // STEP_ROWS,),
                out_shape=jax.ShapeDtypeStruct((chunk_rows, span, width), jnp.float32),
                in_specs=[VMEM] * 5 + [block] * spans,
                out_specs=block,
            )(*prepared, own, *others)
            for own, others in zip(chunks, remote)
        ]
        return updates[0] if CHUNKS == 1 else jnp.concatenate(updates, axis=0)

    return body


def solution(mesh):
    return jax.shard_map(
        make_body(mesh.shape["row"], mesh.shape["chan"]),
        mesh=mesh,
        in_specs=(P("row", "chan", None), P(), P(), P(), P(), P(), P(), P()),
        out_specs=P("row", "chan", None),
        check_vma=False,
    )
```
